256 devices in a mesh: fsdp: 32 (over z_hi, y, core), tensor: 8 (over z_lo, x).
Axes of the slice: x: 4, y: 4, z: 8 (z_hi: 4, z_lo: 2; z = z_hi * 2 + z_lo), core: 2. Of those that a mesh axis runs over, the one named last changes fastest.
Arguments:
- tokens: bfloat16 [4096, 8192], P('fsdp'), may hold values from -6 to 6
- cotangent: bfloat16 [4096, 8192], P('fsdp'), may hold values from -1.5 to 1.5
- gate_blocks: bfloat16 [8, 64, 128, 128], P('tensor', 'fsdp'), may hold values from -0.25 to 0.25
- up_blocks: bfloat16 [8, 64, 128, 128], P('tensor', 'fsdp'), may hold values from -0.25 to 0.25
- down_blocks: bfloat16 [8, 64, 128, 128], P('tensor', 'fsdp'), may hold values from -0.25 to 0.25
- gate_where: int32 [8, 64], P('tensor'), may hold values from 0 to 895, as said below
- up_where: int32 [8, 64], P('tensor'), may hold values from 0 to 895, as said below
- down_where: int32 [8, 64], P('tensor'), may hold values from 0 to 895, as said below
- block_counts: int32 [3, 8], P(None, 'tensor'), may hold values from 32 to 64, as said below
Outputs:
- outputs: bfloat16 [4096, 8192], P('fsdp', 'tensor')
- input_grads: bfloat16 [4096, 8192], P('fsdp', 'tensor')
- gate_grads: bfloat16 [8, 64, 128, 128], P('tensor', 'fsdp')
- up_grads: bfloat16 [8, 64, 128, 128], P('tensor', 'fsdp')
- down_grads: bfloat16 [8, 64, 128, 128], P('tensor', 'fsdp')
The draws below stay inside these ranges and needn't reach their ends.
Inputs may be any that keep to these rules, and one draw needn't show every extreme that they name: Within one group of hidden units the 64 positions of gate_where are distinct. Within one group of hidden units the 64 positions of up_where are distinct. Within one group of hidden units the 64 positions of down_where are distinct. `block_counts`: for each matrix some group has all 64 slots live.
All inputs are finite; a program needn't handle non-finite values.
Results may differ from the reference program's by a relative error of at most 0.015.
Values may be sent and summed in bfloat16 or wider, within the bound.
A program may use at most 128 MiB of HBM per device.

```python
import jax
import jax.numpy as jnp
from jax import lax

D = 8192
FF = 14336
TOK_DEV = 128
NB_DEV = 2
TOKENS = 4096
SLOTS = 64
N_FSDP = 32
N_TENSOR = 8


def where_draw(key, salt):
    cells = D // 128 * (FF // (128 * N_TENSOR))
    keys = jax.random.split(jax.random.fold_in(key, salt), N_TENSOR)
    picked = jax.vmap(lambda single: jax.random.permutation(single, cells)[:NB_DEV * N_FSDP])(keys)
    return picked.astype(jnp.int32)


def draw_gate_where(key, part):
    return where_draw(key, 11)


def draw_up_where(key, part):
    return where_draw(key, 23)


def draw_down_where(key, part):
    return where_draw(key, 37)


def draw_block_counts(key, part):
    slot_count = NB_DEV * N_FSDP
    first, second = jax.random.split(jax.random.fold_in(key, 41))
    drawn = jax.random.randint(first, (3, N_TENSOR), slot_count // 2, slot_count + 1)
    full_shard = jax.random.randint(second, (3, 1), 0, N_TENSOR)
    column = lax.broadcasted_iota(jnp.int32, (3, N_TENSOR), 1)
    return jnp.where(column == full_shard, slot_count, drawn).astype(jnp.int32)


def levels(rng, dims, shards, smallest, high):
    loudness = 1.0
    for axis_at, shards_of in shards:
        heights = jax.random.uniform(jax.random.fold_in(jax.random.fold_in(rng, 6), axis_at), (shards_of,), jnp.float32, smallest / len(shards), high / len(shards))
        loudness = loudness * jnp.repeat(jnp.exp(heights), dims[axis_at] // shards_of).reshape((-1,) + (1,) * (len(dims) - 1 - axis_at))
    return loudness


def scatter_about(own_key, extent, width, reach, pieces=(), held_as=jnp.bfloat16):
    values = width * jax.random.normal(own_key, extent, jnp.float32)
    if pieces:
        values = values * levels(own_key, extent, pieces, -0.22, 0.18)
    return jnp.clip(values, -reach, reach).astype(held_as)


def setup_inputs(seed: int = 0) -> dict:
    key_of = jax.random.split(jax.random.key(seed), 10)
    return {
        "tokens": scatter_about(key_of[0], (TOKENS, D), 1.0, 6.0, ((0, 32),)),
        "cotangent": scatter_about(key_of[1], (TOKENS, D), 0.25, 1.5, ((0, 32),)),
        "gate_blocks": scatter_about(key_of[2], (N_TENSOR, SLOTS, 128, 128), (SLOTS * 16384 * N_TENSOR // FF) ** -0.5, 0.25, ((0, 8), (1, 32))),
        "up_blocks": scatter_about(key_of[3], (N_TENSOR, SLOTS, 128, 128), (SLOTS * 16384 * N_TENSOR // FF) ** -0.5, 0.25, ((0, 8), (1, 32))),
        "down_blocks": scatter_about(key_of[4], (N_TENSOR, SLOTS, 128, 128), (SLOTS * 16384 * N_TENSOR // FF) ** -0.5, 0.25, ((0, 8), (1, 32))),
        "gate_where": draw_gate_where(jax.random.fold_in(key_of[9], 71), 0),
        "up_where": draw_up_where(jax.random.fold_in(key_of[9], 71), 0),
        "down_where": draw_down_where(jax.random.fold_in(key_of[9], 71), 0),
        "block_counts": draw_block_counts(jax.random.fold_in(key_of[9], 71), 0),
    }


def blockwise(pattern, left_side, right_side):
    return jnp.einsum(pattern, left_side.astype(jnp.float32), right_side.astype(jnp.float32), precision=lax.Precision.HIGHEST)


def collect(block_terms, segment_ids, segments):
    return jax.ops.segment_sum(block_terms, segment_ids, num_segments=segments)


def rounded(values):
    return lax.optimization_barrier(values.astype(jnp.bfloat16)).astype(jnp.float32)


def shard_pass(rows_x, rows_g, gate_eff, up_eff, down_eff, gate_where, up_where, down_where, live_parts, row_blocks, col_blocks):
    tok_rows = rows_x.shape[0]
    rows_blocked = rows_x.reshape(tok_rows, row_blocks, 128).transpose(1, 0, 2)
    grad_blocked = rows_g.reshape(tok_rows, row_blocks, 128).transpose(1, 0, 2)
    gate_row = gate_where // col_blocks
    gate_col = gate_where % col_blocks
    up_row = up_where // col_blocks
    up_col = up_where % col_blocks
    down_ff = down_where // row_blocks
    down_d = down_where % row_blocks
    rows_gate = jnp.take(rows_blocked, gate_row, axis=0)
    rows_up = jnp.take(rows_blocked, up_row, axis=0)
    gate_val = collect(blockwise("ntk,nkj->ntj", rows_gate, gate_eff), gate_col, col_blocks)
    up_val = collect(blockwise("ntk,nkj->ntj", rows_up, up_eff), up_col, col_blocks)
    gate_sig = jax.nn.sigmoid(gate_val)
    silu_gate = gate_val * gate_sig
    hidden = (silu_gate * up_val).astype(jnp.bfloat16)
    hidden_sel = jnp.take(hidden, down_ff, axis=0)
    grad_sel = jnp.take(grad_blocked, down_d, axis=0)
    output_term = collect(blockwise("ntk,nkj->ntj", hidden_sel, down_eff), down_d, row_blocks)
    hidden_grad = collect(blockwise("ntj,nkj->ntk", grad_sel, down_eff), down_ff, col_blocks)
    down_part = blockwise("ntk,ntj->nkj", hidden_sel, grad_sel) * live_parts[2]
    gate_delta = (hidden_grad * up_val * gate_sig * (1.0 + gate_val * (1.0 - gate_sig))).astype(jnp.bfloat16)
    up_delta = (hidden_grad * silu_gate).astype(jnp.bfloat16)
    delta_gate = jnp.take(gate_delta, gate_col, axis=0)
    delta_up = jnp.take(up_delta, up_col, axis=0)
    input_term = collect(blockwise("ntj,nkj->ntk", delta_gate, gate_eff), gate_row, row_blocks)
    input_term = input_term + collect(blockwise("ntj,nkj->ntk", delta_up, up_eff), up_row, row_blocks)
    gate_part = blockwise("ntk,ntj->nkj", rows_gate, delta_gate) * live_parts[0]
    up_part = blockwise("ntk,ntj->nkj", rows_up, delta_up) * live_parts[1]
    return output_term, input_term, gate_part, up_part, down_part


def reference(tokens, cotangent, gate_blocks, up_blocks, down_blocks, gate_where, up_where, down_where, block_counts):
    row_blocks = D // 128
    col_blocks = FF // (128 * N_TENSOR)
    slot_count = NB_DEV * N_FSDP
    member_x = tokens.reshape(N_FSDP, TOK_DEV, D)
    member_g = cotangent.reshape(N_FSDP, TOK_DEV, D)
    output_acc = jnp.zeros((N_FSDP, row_blocks, TOK_DEV, 128), jnp.float32)
    input_acc = jnp.zeros((N_FSDP, row_blocks, TOK_DEV, 128), jnp.float32)
    gate_list = []
    up_list = []
    down_list = []
    for tensor_shard in range(N_TENSOR):
        live_slots = lax.broadcasted_iota(jnp.int32, (3, slot_count), 1) < block_counts[:, tensor_shard:tensor_shard + 1]
        live_blocks = live_slots.astype(jnp.bfloat16)[:, :, None, None]
        live_parts = live_slots.astype(jnp.float32)[:, :, None, None]
        gate_eff = gate_blocks[tensor_shard] * live_blocks[0]
        up_eff = up_blocks[tensor_shard] * live_blocks[1]
        down_eff = down_blocks[tensor_shard] * live_blocks[2]

        def per_member(member_rows):
            return shard_pass(member_rows[0], member_rows[1], gate_eff, up_eff, down_eff,
                              gate_where[tensor_shard], up_where[tensor_shard], down_where[tensor_shard],
                              live_parts, row_blocks, col_blocks)

        output_terms, input_terms, gate_parts, up_parts, down_parts = lax.map(per_member, (member_x, member_g))
        output_acc = output_acc + rounded(output_terms)
        input_acc = input_acc + rounded(input_terms)
        gate_list.append(jnp.sum(rounded(gate_parts), axis=0).astype(jnp.bfloat16))
        up_list.append(jnp.sum(rounded(up_parts), axis=0).astype(jnp.bfloat16))
        down_list.append(jnp.sum(rounded(down_parts), axis=0).astype(jnp.bfloat16))
    outputs = output_acc.astype(jnp.bfloat16).transpose(0, 2, 1, 3).reshape(TOKENS, D)
    input_grads = input_acc.astype(jnp.bfloat16).transpose(0, 2, 1, 3).reshape(TOKENS, D)
    return outputs, input_grads, jnp.stack(gate_list), jnp.stack(up_list), jnp.stack(down_list)
```

```python
import jax
import jax.numpy as jnp
from jax import lax
from jax.experimental import pallas as pl
from jax.experimental.pallas import tpu as pltpu
from jax.sharding import PartitionSpec as P

FF = 14336
BK = 128
BF = jnp.bfloat16
F32 = jnp.float32
MESH = pl.DeviceIdType.MESH
VM = pl.BlockSpec(memory_space=pltpu.VMEM)
SM = pl.BlockSpec(memory_space=pltpu.SMEM)
ANY = pl.BlockSpec(memory_space=pl.ANY)
NZ, NY = 4, 4
HALF = (slice(0, 3), slice(3, 6))


class Place:
    def __init__(self):
        rem, div = lax.rem, lax.div
        self.f = lax.axis_index("fsdp")
        self.t = lax.axis_index("tensor")
        self.c = rem(self.f, 2)
        chip = div(self.f, 2)
        y, zh = rem(chip, 4), div(chip, 4)
        self.zl = div(self.t, 4)
        x = rem(self.t, 4)
        self.ys = [rem(y + j, 4) for j in range(4)]
        self.zs = [rem(zh + k, 4) for k in range(4)]
        self.xs = [rem(x + m, 4) for m in range(4)]
        self.same = [[(self.zs[k] * 4 + self.ys[j]) * 2 + self.c for j in range(4)] for k in range(4)]
        self.twin = [[(self.zs[k] * 4 + self.ys[j]) * 2 + (1 - self.c) for j in range(4)] for k in range(4)]
        self.line = [self.zl * 4 + v for v in self.xs]
        self.across = (1 - self.zl) * 4 + x

    def fs(self, k=0, j=0):
        return self.same[k % 4][j % 4]

    def dev(self, k=0, j=0, flip=False):
        return ((self.twin if flip else self.same)[k % 4][j % 4], self.t)

    def tdev(self, m=0, flip=False):
        return (self.f, self.across if flip else self.line[m % 4])


class Sender:
    def __init__(self, sems):
        self.sems = sems
        self.sent = []

    def __call__(self, src, dst, recv, dev):
        copy = pltpu.make_async_remote_copy(
            src_ref=src,
            dst_ref=dst,
            send_sem=self.sems.at[len(self.sent)],
            recv_sem=recv,
            device_id=dev,
            device_id_type=MESH,
        )
        copy.start()
        self.sent.append(copy)

    def finish(self):
        for copy in self.sent:
            copy.wait_send()


def arrive(ref, sem):
    pltpu.make_async_copy(ref, ref, sem).wait()


def meet(devs):
    barrier = pltpu.get_barrier_semaphore()
    for dev in devs:
        pl.semaphore_signal(barrier, inc=1, device_id=dev, device_id_type=MESH)
    pl.semaphore_wait(barrier, len(devs))


ORDER, KEEP, END, SOME = 0, 5, 10, 15
GR, GC, UR, UC, DF, DD = range(20, 26)
GATE, UP, HID, OUT, INP = range(5)
UNROLL = 8
SLOTS = 64
FLOWS = ((0, 2), (4, 1))


def half(fl, h, base=0):
    first, size = FLOWS[fl]
    return pl.ds(base + first + size * h, size)


def whole(fl):
    first, size = FLOWS[fl]
    return pl.ds(first, 2 * size)


def dot_nn(a, b):
    return lax.dot_general(a, b, (((1,), (0,)), ((), ())), preferred_element_type=F32)


def dot_nt(a, b):
    return lax.dot_general(a, b, (((1,), (1,)), ((), ())), preferred_element_type=F32)


def dot_tn(a, b):
    return lax.dot_general(a, b, (((0,), (0,)), ((), ())), preferred_element_type=F32)


def split14(v):
    q = (v * 4682) >> 16
    return q, v - q * 14


def table_kernel(counts, gw, uw, dw, tab):
    n64 = lax.broadcasted_iota(jnp.int32, (1, SLOTS), 1)
    gr, gc = split14(gw[...])
    ur, uc = split14(uw[...])
    df, dd = dw[...] >> 6, dw[...] & 63
    base = (n64 >> 1) * 6 + (n64 & 1)

    def key(k, v):
        return jnp.where(n64 < counts[k], v, 64)

    def wide(v, fill):
        return jnp.concatenate([v, jnp.full((1, SLOTS), fill, jnp.int32)], axis=1)

    keys = (
        wide(key(0, gc), 65),
        wide(key(1, uc), 65),
        wide(key(2, df), 65),
        wide(key(2, dd), 65),
        jnp.concatenate([key(0, gr), key(1, ur)], axis=1),
    )
    loads = (
        wide(n64, 0),
        wide(n64, 0),
        wide(n64, 0),
        wide((base + 4) * 64 + df, 0),
        jnp.concatenate([base * 64 + gc, (base + 2) * 64 + uc + 14], axis=1),
    )
    row_i = lax.broadcasted_iota(jnp.int32, (BK, BK), 0)
    col_i = lax.broadcasted_iota(jnp.int32, (BK, BK), 1)
    lane = lax.broadcasted_iota(jnp.int32, (1, BK), 1)
    for k in range(5):
        by_lane = jnp.broadcast_to(keys[k], (BK, BK))
        by_row = by_lane.T
        code = jnp.broadcast_to(loads[k] * 128 + keys[k], (BK, BK)).T
        before = (by_row < by_lane) | ((by_row == by_lane) & (row_i < col_i))
        rank = jnp.sum(before.astype(jnp.int32), axis=0, keepdims=True)
        rank_row = jnp.broadcast_to(rank, (BK, BK)).T
        both = jnp.sum(jnp.where(rank_row == col_i, code, 0), axis=0, keepdims=True)
        skey = both & 127
        tab[ORDER + k : ORDER + k + 1, :] = both >> 7
        same = (skey == pltpu.roll(skey, 1, 1)) & (lane > 0)
        tab[KEEP + k : KEEP + k + 1, :] = same.astype(jnp.int32)
        upto = jnp.sum((by_row <= col_i).astype(jnp.int32), axis=0, keepdims=True)
        some = jnp.sum((by_row == col_i).astype(jnp.int32), axis=0, keepdims=True)
        tab[END + k : END + k + 1, :] = jnp.maximum(upto - 1, 0)
        tab[SOME + k : SOME + k + 1, :] = (some > 0).astype(jnp.int32)
    for i, v in enumerate((gr, gc, ur, uc, df, dd)):
        tab[GR + i : GR + i + 1, :] = wide(v, 0)


def add2(a, b):
    return (a.astype(F32) + b.astype(F32)).astype(BF)


def add3(a, b, c):
    return a.astype(F32) + b.astype(F32) + c.astype(F32)


def layer_kernel(
    cnt, tab, x_hbm, g_hbm, gate_hbm, up_hbm, down_hbm,
    out_hbm, ing_hbm, gg_hbm, ug_hbm, dg_hbm,
    x, g, w, p, s, hid, delta,
    o, d, pbuf, y2, yr, bbuf, z2, zr, x2, xr, tz, zlb, fin, fing,
    lsem, fsem, ssem, rz, ry, rp, rq, ry2, ryr, rz2, rzr, rx2, rxr, rl,
):
    me = Place()
    own = me.fs()
    cols = hid.shape[0]
    local = [
        pltpu.make_async_copy(src.at[0], w.at[pl.ds(own * 6 + 2 * i, 2)], lsem.at[i])
        for i, src in enumerate((gate_hbm, up_hbm, down_hbm))
    ]
    for copy in local:
        copy.start()

    def bring(b, _):
        at = pl.ds(pl.multiple_of(b * BK, BK), BK)
        pltpu.make_async_copy(x_hbm.at[:, at], x.at[b], lsem.at[3]).start()
        pltpu.make_async_copy(g_hbm.at[:, at], g.at[b], lsem.at[4]).start()
        return 0

    lax.fori_loop(0, x.shape[0], bring, 0)
    meet([me.dev(1), me.dev(3), me.dev(0, 1), me.dev(0, 3), me.dev(flip=True),
          me.tdev(1), me.tdev(3), me.tdev(flip=True)])
    for copy in local:
        copy.wait()
    send = Sender(ssem)

    def piece(k, j, fl, h):
        return w.at[half(fl, h, me.fs(k, j) * 6)]

    def to_z(k, fl, h, step):
        send(piece(k, 0, fl, h), piece(k, 0, fl, h), rz.at[fl, (k - step) % 4, h], me.dev(step))

    def to_y(k, j, fl, h, step):
        send(piece(k, j, fl, h), piece(k, j, fl, h), ry.at[fl, k, (j - step) % 4, h], me.dev(0, step))

    def to_core(k, j, fl, h):
        send(piece(k, j, fl, h), piece(k, j, fl, h), rp.at[fl, k, j, h], me.dev(flip=True))

    def on_y(k, j, fl):
        for h in (0, 1):
            arrive(piece(k, j, fl, h), ry.at[fl, k, j, h])
            if j == 3 and h == 0:
                to_y(k, j, fl, h, 1)
            if j == 1 and h == 1:
                to_y(k, j, fl, h, -1)
            to_core(k, j, fl, h)

    def on_z(k, fl):
        for h in (0, 1):
            arrive(piece(k, 0, fl, h), rz.at[fl, k, h])
            if k == 3 and h == 0:
                to_z(k, fl, h, 1)
            if k == 1 and h == 1:
                to_z(k, fl, h, -1)
            to_y(k, 0, fl, h, 1)
            to_y(k, 0, fl, h, -1)
            to_core(k, 0, fl, h)

    def begin(fl):
        for h in (0, 1):
            to_z(0, fl, h, 1)
            to_z(0, fl, h, -1)
            to_y(0, 0, fl, h, 1)
            to_y(0, 0, fl, h, -1)
            to_core(0, 0, fl, h)

    def products(f, fl):
        for slot in (0, 1):
            n = 2 * f + slot
            if fl == 0:
                p[n] = dot_nn(x[tab[GR, n]], w[f * 6 + slot])
                p[SLOTS + n] = dot_nn(x[tab[UR, n]], w[f * 6 + 2 + slot])
            else:
                p[2 * SLOTS + n] = dot_nt(g[tab[DD, n]], w[f * 6 + 4 + slot])

    def mine(chunks, fl):
        for k, j in chunks:
            products(me.fs(k, j), fl)

    def theirs(chunks, fl):
        for k, j in chunks:
            f = me.twin[k][j]
            for h in (0, 1):
                arrive(w.at[half(fl, h, f * 6)], rp.at[fl, k, j, h])
        for k, j in chunks:
            products(me.twin[k][j], fl)

    groups = (
        ((0, 0),),
        ((0, 3), (0, 1), (3, 0), (1, 0)),
        ((2, 0), (0, 2)),
        ((3, 3), (3, 1), (1, 3), (1, 1)),
        ((3, 2), (1, 2)),
        ((2, 3), (2, 1)),
        ((2, 2),),
    )

    def take(i, fl):
        for k, j in groups[i]:
            if j == 0:
                on_z(k, fl)
            else:
                on_y(k, j, fl)

    def run(kind, count, first, term):
        def body(step, acc):
            for u in range(UNROLL):
                i = step * UNROLL + u
                keep = tab[KEEP + kind, i].astype(F32)
                acc = acc * keep + term(tab[ORDER + kind, i])
                s[first + i] = acc
            return acc

        lax.fori_loop(0, count // UNROLL, body, jnp.zeros((BK, BK), F32))

    def pick(first, kind, c):
        return s[first + tab[END + kind, c]] * tab[SOME + kind, c].astype(F32)

    begin(0)
    arrive(x, lsem.at[3])
    arrive(g, lsem.at[4])
    mine(groups[0], 0)
    for i in range(1, 7):
        take(i, 0)
        if i == 4:
            begin(1)
        mine(groups[i], 0)
        theirs(groups[i - 1], 0)
    mine(groups[0], 1)
    take(1, 1)
    theirs(groups[6], 0)
    run(GATE, SLOTS, 0, lambda n: p[n])
    take(2, 1)
    take(3, 1)
    run(UP, SLOTS, SLOTS, lambda n: p[SLOTS + n])
    mine(groups[1], 1)
    theirs(groups[0], 1)
    take(4, 1)

    def act(c, _):
        gate = pick(0, GATE, c)
        up = pick(SLOTS, UP, c)
        sig = jax.nn.sigmoid(gate)
        silu = gate * sig
        hid[c] = (silu * up).astype(BF)
        p[c] = up * sig * (1.0 + gate * (1.0 - sig))
        p[cols + c] = silu
        return 0

    lax.fori_loop(0, cols, act, 0)
    take(5, 1)
    mine(groups[2] + groups[3], 1)
    theirs(groups[1], 1)
    take(6, 1)
    mine(groups[4] + groups[5] + groups[6], 1)
    theirs(groups[2] + groups[3], 1)
    theirs(groups[4] + groups[5] + groups[6], 1)

    def opiece(a, zl, m):
        return o.at[a, zl * 4 + me.xs[m % 4]]

    def put(a, first, kind):
        def body(q, _):
            for r in range(8):
                o[a, q, :, r * BK : (r + 1) * BK] = pick(first, kind, q * 8 + r).astype(BF)
            return 0

        lax.fori_loop(0, 8, body, 0)

    def x_start(a):
        send(opiece(a, 0, 2), x2.at[a, 0], rx2.at[a, 0], me.tdev(1))
        send(opiece(a, 1, 2), x2.at[a, 1], rx2.at[a, 1], me.tdev(-1))
        send(opiece(a, 1, 1), xr.at[a, 0, 1], rxr.at[a, 0, 1], me.tdev(1))
        send(opiece(a, 0, -1), xr.at[a, 1, 0], rxr.at[a, 1, 0], me.tdev(-1))

    def x_pass(a):
        for h, m in ((0, 1), (1, -1)):
            arrive(x2.at[a, h], rx2.at[a, h])
            x2[a, h] = add2(o[a, h * 4 + me.xs[m % 4]], x2[a, h])
            send(x2.at[a, h], xr.at[a, h, h], rxr.at[a, h, h], me.tdev(m))

    def x_end(a):
        for e in (0, 1):
            for h in (0, 1):
                arrive(xr.at[a, e, h], rxr.at[a, e, h])
        other = 1 - me.zl
        tz[a] = add3(o[a, me.across], xr[a, 0, other], xr[a, 1, other]).astype(BF)
        send(tz.at[a], zlb.at[a], rl.at[a], me.tdev(flip=True))

    results = []

    def result(src, dst):
        copy = pltpu.make_async_copy(src, dst, fsem.at[len(results)])
        copy.start()
        results.append(copy)

    def l_end(a):
        own_sum = add3(o[a, me.line[0]], xr[a, 0, me.zl], xr[a, 1, me.zl])
        arrive(zlb.at[a], rl.at[a])
        fin[a] = (own_sum + zlb[a].astype(F32)).astype(BF)
        result(fin.at[a], (out_hbm, ing_hbm)[a])

    def core_send(k, fl):
        for j in (2, 1, 3, 0):
            send(d.at[me.twin[k][j], whole(fl)], pbuf.at[k, j, whole(fl)], rq.at[fl, k, j], me.dev(flip=True))

    def core_sum(k, j, fl):
        arrive(pbuf.at[k, j, whole(fl)], rq.at[fl, k, j])
        f = me.fs(k, j)
        d[f, whole(fl)] = add2(d[f, whole(fl)], pbuf[k, j, whole(fl)])

    def y_start(k, fl):
        core_sum(k, 2, fl)
        far = me.fs(k, 2)
        send(d.at[far, half(fl, 0)], y2.at[k, half(fl, 0)], ry2.at[fl, k, 0], me.dev(0, 1))
        send(d.at[far, half(fl, 1)], y2.at[k, half(fl, 1)], ry2.at[fl, k, 1], me.dev(0, -1))
        core_sum(k, 1, fl)
        send(d.at[me.fs(k, 1), half(fl, 1)], yr.at[k, 0, half(fl, 1)], ryr.at[fl, k, 0, 1], me.dev(0, 1))
        core_sum(k, 3, fl)
        send(d.at[me.fs(k, 3), half(fl, 0)], yr.at[k, 1, half(fl, 0)], ryr.at[fl, k, 1, 0], me.dev(0, -1))
        core_sum(k, 0, fl)

    def y_pass(k, fl):
        for h, j in ((0, 1), (1, 3)):
            at = half(fl, h)
            arrive(y2.at[k, at], ry2.at[fl, k, h])
            y2[k, at] = add2(d[me.fs(k, j), at], y2[k, at])
            send(y2.at[k, at], yr.at[k, h, at], ryr.at[fl, k, h, h], me.dev(0, j))

    def y_end(k, fl):
        for e in (0, 1):
            for h in (0, 1):
                arrive(yr.at[k, e, half(fl, h)], ryr.at[fl, k, e, h])
        at = whole(fl)
        bbuf[k, at] = add3(d[me.fs(k, 0), at], yr[k, 0, at], yr[k, 1, at]).astype(BF)
        if k == 2:
            send(bbuf.at[2, half(fl, 0)], z2.at[half(fl, 0)], rz2.at[fl, 0], me.dev(1))
            send(bbuf.at[2, half(fl, 1)], z2.at[half(fl, 1)], rz2.at[fl, 1], me.dev(-1))
        if k == 1:
            send(bbuf.at[1, half(fl, 1)], zr.at[0, half(fl, 1)], rzr.at[fl, 0, 1], me.dev(1))
        if k == 3:
            send(bbuf.at[3, half(fl, 0)], zr.at[1, half(fl, 0)], rzr.at[fl, 1, 0], me.dev(-1))

    def z_pass(fl):
        for h, k in ((0, 1), (1, 3)):
            at = half(fl, h)
            arrive(z2.at[at], rz2.at[fl, h])
            z2[at] = add2(bbuf[k, at], z2[at])
            send(z2.at[at], zr.at[h, at], rzr.at[fl, h, h], me.dev(k))

    def z_end(fl):
        for e in (0, 1):
            for h in (0, 1):
                arrive(zr.at[e, half(fl, h)], rzr.at[fl, e, h])
        at = whole(fl)
        fing[at] = add3(bbuf[0, at], zr[0, at], zr[1, at]).astype(BF)
        for b in (0, 1) if fl == 0 else (2,):
            result(fing.at[pl.ds(2 * b, 2)], (gg_hbm, ug_hbm, dg_hbm)[b].at[0])

    def live(k, n):
        return (n < cnt[k]).astype(F32)

    def down_grads(f, _):
        for slot in (0, 1):
            n = 2 * f + slot
            d[f, 4 + slot] = (dot_tn(hid[tab[DF, n]], g[tab[DD, n]]) * live(2, n)).astype(BF)
        return 0

    def in_grads(k):
        def body(i, _):
            f = me.zs[k] * 8 + i
            for slot in (0, 1):
                n = 2 * f + slot
                d[f, slot] = (dot_tn(x[tab[GR, n]], delta[tab[GC, n]]) * live(0, n)).astype(BF)
                d[f, 2 + slot] = (dot_tn(x[tab[UR, n]], delta[cols + tab[UC, n]]) * live(1, n)).astype(BF)
            return 0

        lax.fori_loop(0, 8, body, 0)
        core_send(k, 0)

    run(OUT, SLOTS, 0, lambda v: dot_nn(hid[v & 63], w[v >> 6]))
    put(0, 0, OUT)
    x_start(0)
    lax.fori_loop(0, 32, down_grads, 0)
    for k in (2, 1, 3, 0):
        core_send(k, 1)
    run(HID, SLOTS, 2 * SLOTS, lambda n: p[2 * SLOTS + n])

    def act_grad(c, _):
        hg = pick(2 * SLOTS, HID, c)
        delta[c] = (hg * p[c]).astype(BF)
        delta[cols + c] = (hg * p[cols + c]).astype(BF)
        return 0

    lax.fori_loop(0, cols, act_grad, 0)
    for k in (2, 1, 3, 0):
        y_start(k, 1)
    run(INP, 2 * SLOTS, SLOTS, lambda v: dot_nt(delta[v & 63], w[v >> 6]))
    put(1, SLOTS, INP)
    x_start(1)
    in_grads(2)
    x_pass(0)
    in_grads(1)
    y_start(2, 0)
    in_grads(3)
    y_start(1, 0)
    in_grads(0)
    y_start(3, 0)
    for k in (2, 1, 3, 0):
        y_pass(k, 1)
    y_start(0, 0)
    for k in (2, 1, 3, 0):
        y_end(k, 1)
    y_pass(2, 0)
    z_pass(1)
    x_end(0)
    y_pass(1, 0)
    y_pass(3, 0)
    y_end(2, 0)
    x_pass(1)
    y_pass(0, 0)
    y_end(1, 0)
    z_end(1)
    l_end(0)
    y_end(3, 0)
    z_pass(0)
    y_end(0, 0)
    x_end(1)
    z_end(0)
    l_end(1)
    for copy in results:
        copy.wait()
    send.finish()


def finish_kernel(*refs):
    for src, dst in zip(refs[:5], refs[5:]):
        dst[...] = src[...]


def shards(tokens, cotangent, gate_blocks, up_blocks, down_blocks, gate_where, up_where, down_where, block_counts):
    cols = FF // (BK * lax.axis_size("tensor"))
    toks = tokens.shape[0]
    dma = pltpu.SemaphoreType.DMA
    shapes = (
        jax.ShapeDtypeStruct((toks, 1024), BF),
        jax.ShapeDtypeStruct((toks, 1024), BF),
        jax.ShapeDtypeStruct((1, 2, BK, BK), BF),
        jax.ShapeDtypeStruct((1, 2, BK, BK), BF),
        jax.ShapeDtypeStruct((1, 2, BK, BK), BF),
    )
    counts = block_counts.reshape(3)
    table = pl.pallas_call(
        table_kernel,
        out_shape=jax.ShapeDtypeStruct((26, BK), jnp.int32),
        in_specs=[SM, VM, VM, VM],
        out_specs=VM,
    )(counts, gate_where, up_where, down_where)
    results = pl.pallas_call(
        layer_kernel,
        out_shape=shapes,
        in_specs=[SM, SM] + [ANY] * 5,
        out_specs=(ANY,) * 5,
        scratch_shapes=[
            pltpu.VMEM((tokens.shape[1] // BK, toks, BK), BF),
            pltpu.VMEM((tokens.shape[1] // BK, toks, BK), BF),
            pltpu.VMEM((192, BK, BK), BF),
            pltpu.VMEM((3 * SLOTS, BK, BK), F32),
            pltpu.VMEM((3 * SLOTS, BK, BK), F32),
            pltpu.VMEM((cols, BK, BK), BF),
            pltpu.VMEM((2 * cols, BK, BK), BF),
            pltpu.VMEM((2, 8, toks, 1024), BF),
            pltpu.VMEM((32, 6, BK, BK), BF),
            pltpu.VMEM((4, 4, 6, BK, BK), BF),
            pltpu.VMEM((4, 6, BK, BK), BF),
            pltpu.VMEM((4, 2, 6, BK, BK), BF),
            pltpu.VMEM((4, 6, BK, BK), BF),
            pltpu.VMEM((6, BK, BK), BF),
            pltpu.VMEM((2, 6, BK, BK), BF),
            pltpu.VMEM((2, 2, toks, 1024), BF),
            pltpu.VMEM((2, 2, 2, toks, 1024), BF),
            pltpu.VMEM((2, toks, 1024), BF),
            pltpu.VMEM((2, toks, 1024), BF),
            pltpu.VMEM((2, toks, 1024), BF),
            pltpu.VMEM((6, BK, BK), BF),
            dma((5,)),
            dma((5,)),
            dma((240,)),
            dma((2, 4, 2)),
            dma((2, 4, 4, 2)),
            dma((2, 4, 4, 2)),
            dma((2, 4, 4)),
            dma((2, 4, 2)),
            dma((2, 4, 2, 2)),
            dma((2, 2)),
            dma((2, 2, 2)),
            dma((2, 2)),
            dma((2, 2, 2)),
            dma((2,)),
        ],
        compiler_params=pltpu.CompilerParams(
            collective_id=0, has_side_effects=True, vmem_limit_bytes=67043328
        ),
    )(
        counts, table, tokens, cotangent, gate_blocks, up_blocks, down_blocks,
    )
    return pl.pallas_call(
        finish_kernel, out_shape=shapes, in_specs=[VM] * 5, out_specs=(VM,) * 5,
    )(*results)


def solution(mesh):
    placed = (
        P("fsdp", None),
        P("fsdp", None),
        P("tensor", "fsdp", None, None),
        P("tensor", "fsdp", None, None),
        P("tensor", "fsdp", None, None),
        P("tensor", None),
        P("tensor", None),
        P("tensor", None),
        P(None, "tensor"),
    )
    return jax.shard_map(
        shards,
        mesh=mesh,
        in_specs=placed,
        out_specs=(
            P("fsdp", "tensor"),
            P("fsdp", "tensor"),
            P("tensor", "fsdp", None, None),
            P("tensor", "fsdp", None, None),
            P("tensor", "fsdp", None, None),
        ),
        check_vma=False,
    )
```

```python
import jax
import jax.numpy as jnp
from jax import lax
from jax.experimental import pallas as pl
from jax.experimental.pallas import tpu as pltpu
from jax.sharding import PartitionSpec as P

FF = 14336
BK = 128
BF = jnp.bfloat16
F32 = jnp.float32
MESH = pl.DeviceIdType.MESH
VM = pl.BlockSpec(memory_space=pltpu.VMEM)
SM = pl.BlockSpec(memory_space=pltpu.SMEM)
ANY = pl.BlockSpec(memory_space=pl.ANY)
NZ, NY = 4, 4
HALF = (slice(0, 3), slice(3, 6))


class Place:
    def __init__(self):
        rem, div = lax.rem, lax.div
        self.f = lax.axis_index("fsdp")
        self.t = lax.axis_index("tensor")
        self.c = rem(self.f, 2)
        chip = div(self.f, 2)
        y, zh = rem(chip, 4), div(chip, 4)
        self.zl = div(self.t, 4)
        x = rem(self.t, 4)
        self.ys = [rem(y + j, 4) for j in range(4)]
        self.zs = [rem(zh + k, 4) for k in range(4)]
        self.xs = [rem(x + m, 4) for m in range(4)]
        self.same = [[(self.zs[k] * 4 + self.ys[j]) * 2 + self.c for j in range(4)] for k in range(4)]
        self.twin = [[(self.zs[k] * 4 + self.ys[j]) * 2 + (1 - self.c) for j in range(4)] for k in range(4)]
        self.line = [self.zl * 4 + v for v in self.xs]
        self.across = (1 - self.zl) * 4 + x

    def fs(self, k=0, j=0):
        return self.same[k % 4][j % 4]

    def dev(self, k=0, j=0, flip=False):
        return ((self.twin if flip else self.same)[k % 4][j % 4], self.t)

    def tdev(self, m=0, flip=False):
        return (self.f, self.across if flip else self.line[m % 4])


class Sender:
    def __init__(self, sems):
        self.sems = sems
        self.sent = []

    def __call__(self, src, dst, recv, dev):
        copy = pltpu.make_async_remote_copy(
            src_ref=src,
            dst_ref=dst,
            send_sem=self.sems.at[len(self.sent)],
            recv_sem=recv,
            device_id=dev,
            device_id_type=MESH,
        )
        copy.start()
        self.sent.append(copy)

    def finish(self):
        for copy in self.sent:
            copy.wait_send()


def arrive(ref, sem):
    pltpu.make_async_copy(ref, ref, sem).wait()


def meet(devs):
    barrier = pltpu.get_barrier_semaphore()
    for dev in devs:
        pl.semaphore_signal(barrier, inc=1, device_id=dev, device_id_type=MESH)
    pl.semaphore_wait(barrier, len(devs))


ORDER, KEEP, END, SOME = 0, 5, 10, 15
GR, GC, UR, UC, DF, DD = range(20, 26)
GATE, UP, HID, OUT, INP = range(5)
UNROLL = 8
SLOTS = 64
FLOWS = ((0, 2), (4, 1))


def half(fl, h, base=0):
    first, size = FLOWS[fl]
    return pl.ds(base + first + size * h, size)


def whole(fl):
    first, size = FLOWS[fl]
    return pl.ds(first, 2 * size)


def dot_nn(a, b):
    return lax.dot_general(a, b, (((1,), (0,)), ((), ())), preferred_element_type=F32)


def dot_nt(a, b):
    return lax.dot_general(a, b, (((1,), (1,)), ((), ())), preferred_element_type=F32)


def dot_tn(a, b):
    return lax.dot_general(a, b, (((0,), (0,)), ((), ())), preferred_element_type=F32)


def split14(v):
    q = (v * 4682) >> 16
    return q, v - q * 14


def table_kernel(counts, gw, uw, dw, tab):
    n64 = lax.broadcasted_iota(jnp.int32, (1, SLOTS), 1)
    gr, gc = split14(gw[...])
    ur, uc = split14(uw[...])
    df, dd = dw[...] >> 6, dw[...] & 63
    base = (n64 >> 1) * 6 + (n64 & 1)

    def key(k, v):
        return jnp.where(n64 < counts[k], v, 64)

    def wide(v, fill):
        return jnp.concatenate([v, jnp.full((1, SLOTS), fill, jnp.int32)], axis=1)

    keys = (
        wide(key(0, gc), 65),
        wide(key(1, uc), 65),
        wide(key(2, df), 65),
        wide(key(2, dd), 65),
        jnp.concatenate([key(0, gr), key(1, ur)], axis=1),
    )
    loads = (
        wide(n64, 0),
        wide(n64, 0),
        wide(n64, 0),
        wide((base + 4) * 64 + df, 0),
        jnp.concatenate([base * 64 + gc, (base + 2) * 64 + uc + 14], axis=1),
    )
    row_i = lax.broadcasted_iota(jnp.int32, (BK, BK), 0)
    col_i = lax.broadcasted_iota(jnp.int32, (BK, BK), 1)
    lane = lax.broadcasted_iota(jnp.int32, (1, BK), 1)
    for k in range(5):
        by_lane = jnp.broadcast_to(keys[k], (BK, BK))
        by_row = by_lane.T
        code = jnp.broadcast_to(loads[k] * 128 + keys[k], (BK, BK)).T
        before = (by_row < by_lane) | ((by_row == by_lane) & (row_i < col_i))
        rank = jnp.sum(before.astype(jnp.int32), axis=0, keepdims=True)
        rank_row = jnp.broadcast_to(rank, (BK, BK)).T
        both = jnp.sum(jnp.where(rank_row == col_i, code, 0), axis=0, keepdims=True)
        skey = both & 127
        tab[ORDER + k : ORDER + k + 1, :] = both >> 7
        same = (skey == pltpu.roll(skey, 1, 1)) & (lane > 0)
        tab[KEEP + k : KEEP + k + 1, :] = same.astype(jnp.int32)
        upto = jnp.sum((by_row <= col_i).astype(jnp.int32), axis=0, keepdims=True)
        some = jnp.sum((by_row == col_i).astype(jnp.int32), axis=0, keepdims=True)
        tab[END + k : END + k + 1, :] = jnp.maximum(upto - 1, 0)
        tab[SOME + k : SOME + k + 1, :] = (some > 0).astype(jnp.int32)
    for i, v in enumerate((gr, gc, ur, uc, df, dd)):
        tab[GR + i : GR + i + 1, :] = wide(v, 0)


def add2(a, b):
    return (a.astype(F32) + b.astype(F32)).astype(BF)


def add3(a, b, c):
    return a.astype(F32) + b.astype(F32) + c.astype(F32)


def layer_kernel(
    cnt, tab, x_hbm, g_hbm, gate_hbm, up_hbm, down_hbm,
    out_hbm, ing_hbm, gg_hbm, ug_hbm, dg_hbm,
    x, g, w, p, s, hid, delta,
    o, d, pbuf, y2, yr, bbuf, z2, zr, x2, xr, tz, zlb, fin, fing,
    lsem, fsem, ssem, rz, ry, rp, rq, ry2, ryr, rz2, rzr, rx2, rxr, rl,
):
    me = Place()
    own = me.fs()
    cols = hid.shape[0]
    local = [
        pltpu.make_async_copy(src.at[0], w.at[pl.ds(own * 6 + 2 * i, 2)], lsem.at[i])
        for i, src in enumerate((gate_hbm, up_hbm, down_hbm))
    ]
    for copy in local:
        copy.start()

    def bring(b, _):
        at = pl.ds(pl.multiple_of(b * BK, BK), BK)
        pltpu.make_async_copy(x_hbm.at[:, at], x.at[b], lsem.at[3]).start()
        pltpu.make_async_copy(g_hbm.at[:, at], g.at[b], lsem.at[4]).start()
        return 0

    lax.fori_loop(0, x.shape[0], bring, 0)
    meet([me.dev(1), me.dev(3), me.dev(0, 1), me.dev(0, 3), me.dev(flip=True),
          me.tdev(1), me.tdev(3), me.tdev(flip=True)])
    for copy in local:
        copy.wait()
    send = Sender(ssem)

    def piece(k, j, fl, h):
        return w.at[half(fl, h, me.fs(k, j) * 6)]

    def to_z(k, fl, h, step):
        send(piece(k, 0, fl, h), piece(k, 0, fl, h), rz.at[fl, (k - step) % 4, h], me.dev(step))

    def to_y(k, j, fl, h, step):
        send(piece(k, j, fl, h), piece(k, j, fl, h), ry.at[fl, k, (j - step) % 4, h], me.dev(0, step))

    def to_core(k, j, fl, h):
        send(piece(k, j, fl, h), piece(k, j, fl, h), rp.at[fl, k, j, h], me.dev(flip=True))

    def on_y(k, j, fl):
        for h in (0, 1):
            arrive(piece(k, j, fl, h), ry.at[fl, k, j, h])
            if j == 3 and h == 0:
                to_y(k, j, fl, h, 1)
            if j == 1 and h == 1:
                to_y(k, j, fl, h, -1)
            to_core(k, j, fl, h)

    def on_z(k, fl):
        for h in (0, 1):
            arrive(piece(k, 0, fl, h), rz.at[fl, k, h])
            if k == 3 and h == 0:
                to_z(k, fl, h, 1)
            if k == 1 and h == 1:
                to_z(k, fl, h, -1)
            to_y(k, 0, fl, h, 1)
            to_y(k, 0, fl, h, -1)
            to_core(k, 0, fl, h)

    def begin(fl):
        for h in (0, 1):
            to_z(0, fl, h, 1)
            to_z(0, fl, h, -1)
            to_y(0, 0, fl, h, 1)
            to_y(0, 0, fl, h, -1)
            to_core(0, 0, fl, h)

    def products(f, fl):
        for slot in (0, 1):
            n = 2 * f + slot
            if fl == 0:
                p[n] = dot_nn(x[tab[GR, n]], w[f * 6 + slot])
                p[SLOTS + n] = dot_nn(x[tab[UR, n]], w[f * 6 + 2 + slot])
            else:
                p[2 * SLOTS + n] = dot_nt(g[tab[DD, n]], w[f * 6 + 4 + slot])

    def mine(chunks, fl):
        for k, j in chunks:
            products(me.fs(k, j), fl)

    def wait_theirs(chunks, fl):
        for k, j in chunks:
            for h in (0, 1):
                arrive(w.at[half(fl, h, me.twin[k][j] * 6)], rp.at[fl, k, j, h])

    def theirs(chunks, fl, wait=True):
        if wait:
            wait_theirs(chunks, fl)
        for k, j in chunks:
            products(me.twin[k][j], fl)

    groups = (
        ((0, 0),),
        ((0, 3), (0, 1), (3, 0), (1, 0)),
        ((2, 0), (0, 2)),
        ((3, 3), (3, 1), (1, 3), (1, 1)),
        ((3, 2), (1, 2)),
        ((2, 3), (2, 1)),
        ((2, 2),),
    )

    def take(i, fl):
        for k, j in groups[i]:
            if j == 0:
                on_z(k, fl)
            else:
                on_y(k, j, fl)

    def run(kind, count, first, term):
        def body(step, acc):
            for u in range(UNROLL):
                i = step * UNROLL + u
                keep = tab[KEEP + kind, i].astype(F32)
                acc = acc * keep + term(tab[ORDER + kind, i])
                s[first + i] = acc
            return acc

        lax.fori_loop(0, count // UNROLL, body, jnp.zeros((BK, BK), F32))

    def pick(first, kind, c):
        return s[first + tab[END + kind, c]] * tab[SOME + kind, c].astype(F32)

    begin(0)
    begin(1)
    take(1, 0)
    arrive(x, lsem.at[3])
    mine(groups[0] + groups[1], 0)
    take(2, 0)
    take(1, 1)
    theirs(groups[0], 0)
    mine(groups[2], 0)
    take(3, 0)
    take(2, 1)
    theirs(groups[1], 0)
    mine(groups[3], 0)
    take(4, 0)
    theirs(groups[2], 0)
    mine(groups[4], 0)
    take(5, 0)
    take(3, 1)
    theirs(groups[3], 0)
    mine(groups[5], 0)
    take(6, 0)
    theirs(groups[4], 0)
    mine(groups[6], 0)
    take(4, 1)
    theirs(groups[5] + groups[6], 0)
    run(GATE, SLOTS, 0, lambda n: p[n])
    run(UP, SLOTS, SLOTS, lambda n: p[SLOTS + n])

    def act(c, _):
        gate = pick(0, GATE, c)
        up = pick(SLOTS, UP, c)
        sig = jax.nn.sigmoid(gate)
        silu = gate * sig
        hid[c] = (silu * up).astype(BF)
        p[c] = up * sig * (1.0 + gate * (1.0 - sig))
        p[cols + c] = silu
        return 0

    lax.fori_loop(0, cols, act, 0)
    take(5, 1)
    arrive(g, lsem.at[4])
    mine(groups[0] + groups[1] + groups[2], 1)
    take(6, 1)
    wait_theirs(sum(groups, ()), 1)

    def opiece(b, zl, m):
        return o.at[b, zl * 4 + me.xs[m % 4]]

    def put(a, first, kind):
        def body(q, _):
            for r in range(8):
                at = slice(r % 4 * BK, (r % 4 + 1) * BK)
                o[2 * a + r // 4, q, :, at] = pick(first, kind, q * 8 + r).astype(BF)
            return 0

        lax.fori_loop(0, 8, body, 0)

    def x_start(a):
        for b in (2 * a, 2 * a + 1):
            send(opiece(b, 0, 2), x2.at[b, 0], rx2.at[b, 0], me.tdev(1))
            send(opiece(b, 1, 2), x2.at[b, 1], rx2.at[b, 1], me.tdev(-1))
        for b in (2 * a, 2 * a + 1):
            send(opiece(b, 1, 1), xr.at[b, 0, 1], rxr.at[b, 0, 1], me.tdev(1))
            send(opiece(b, 0, -1), xr.at[b, 1, 0], rxr.at[b, 1, 0], me.tdev(-1))

    def x_pass(b):
        for h, m in ((0, 1), (1, -1)):
            arrive(x2.at[b, h], rx2.at[b, h])
            x2[b, h] = add2(o[b, h * 4 + me.xs[m % 4]], x2[b, h])
            send(x2.at[b, h], xr.at[b, h, h], rxr.at[b, h, h], me.tdev(m))

    def x_end(b):
        for e in (0, 1):
            for h in (0, 1):
                arrive(xr.at[b, e, h], rxr.at[b, e, h])
        other = 1 - me.zl
        tz[b] = add3(o[b, me.across], xr[b, 0, other], xr[b, 1, other]).astype(BF)
        send(tz.at[b], zlb.at[b], rl.at[b], me.tdev(flip=True))

    results = []

    def result(src, dst):
        copy = pltpu.make_async_copy(src, dst, fsem.at[len(results)])
        copy.start()
        results.append(copy)

    def l_end(b):
        own_sum = add3(o[b, me.line[0]], xr[b, 0, me.zl], xr[b, 1, me.zl])
        arrive(zlb.at[b], rl.at[b])
        fin[b] = (own_sum + zlb[b].astype(F32)).astype(BF)
        result(fin.at[b], (out_hbm, ing_hbm)[b // 2].at[:, pl.ds(b % 2 * 512, 512)])

    def core_send(k, fl):
        for j in (2, 1, 3, 0):
            send(d.at[me.twin[k][j], whole(fl)], pbuf.at[k, j, whole(fl)], rq.at[fl, k, j], me.dev(flip=True))

    def core_sum(k, j, fl):
        arrive(pbuf.at[k, j, whole(fl)], rq.at[fl, k, j])
        f = me.fs(k, j)
        d[f, whole(fl)] = add2(d[f, whole(fl)], pbuf[k, j, whole(fl)])

    def y_start(k, fl):
        core_sum(k, 2, fl)
        far = me.fs(k, 2)
        send(d.at[far, half(fl, 0)], y2.at[k, half(fl, 0)], ry2.at[fl, k, 0], me.dev(0, 1))
        send(d.at[far, half(fl, 1)], y2.at[k, half(fl, 1)], ry2.at[fl, k, 1], me.dev(0, -1))
        core_sum(k, 1, fl)
        send(d.at[me.fs(k, 1), half(fl, 1)], yr.at[k, 0, half(fl, 1)], ryr.at[fl, k, 0, 1], me.dev(0, 1))
        core_sum(k, 3, fl)
        send(d.at[me.fs(k, 3), half(fl, 0)], yr.at[k, 1, half(fl, 0)], ryr.at[fl, k, 1, 0], me.dev(0, -1))
        core_sum(k, 0, fl)

    def y_pass(k, fl):
        for h, j in ((0, 1), (1, 3)):
            at = half(fl, h)
            arrive(y2.at[k, at], ry2.at[fl, k, h])
            y2[k, at] = add2(d[me.fs(k, j), at], y2[k, at])
            send(y2.at[k, at], yr.at[k, h, at], ryr.at[fl, k, h, h], me.dev(0, j))

    def y_end(k, fl):
        for e in (0, 1):
            for h in (0, 1):
                arrive(yr.at[k, e, half(fl, h)], ryr.at[fl, k, e, h])
        at = whole(fl)
        bbuf[k, at] = add3(d[me.fs(k, 0), at], yr[k, 0, at], yr[k, 1, at]).astype(BF)
        if k == 2:
            send(bbuf.at[2, half(fl, 0)], z2.at[half(fl, 0)], rz2.at[fl, 0], me.dev(1))
            send(bbuf.at[2, half(fl, 1)], z2.at[half(fl, 1)], rz2.at[fl, 1], me.dev(-1))
        if k == 1:
            send(bbuf.at[1, half(fl, 1)], zr.at[0, half(fl, 1)], rzr.at[fl, 0, 1], me.dev(1))
        if k == 3:
            send(bbuf.at[3, half(fl, 0)], zr.at[1, half(fl, 0)], rzr.at[fl, 1, 0], me.dev(-1))

    def z_pass(fl):
        for h, k in ((0, 1), (1, 3)):
            at = half(fl, h)
            arrive(z2.at[at], rz2.at[fl, h])
            z2[at] = add2(bbuf[k, at], z2[at])
            send(z2.at[at], zr.at[h, at], rzr.at[fl, h, h], me.dev(k))

    def z_end(fl):
        for e in (0, 1):
            for h in (0, 1):
                arrive(zr.at[e, half(fl, h)], rzr.at[fl, e, h])
        at = whole(fl)
        fing[at] = add3(bbuf[0, at], zr[0, at], zr[1, at]).astype(BF)
        for b in (0, 1) if fl == 0 else (2,):
            result(fing.at[pl.ds(2 * b, 2)], (gg_hbm, ug_hbm, dg_hbm)[b].at[0])

    def live(k, n):
        return (n < cnt[k]).astype(F32)

    def down_grads(i, _):
        for e in range(4):
            f = i * 4 + e
            for slot in (0, 1):
                n = 2 * f + slot
                d[f, 4 + slot] = (dot_tn(hid[tab[DF, n]], g[tab[DD, n]]) * live(2, n)).astype(BF)
        return 0

    def in_grads(k):
        def body(i, _):
            for e in (0, 1):
                f = me.zs[k] * 8 + i * 2 + e
                for slot in (0, 1):
                    n = 2 * f + slot
                    d[f, slot] = (dot_tn(x[tab[GR, n]], delta[tab[GC, n]]) * live(0, n)).astype(BF)
                    d[f, 2 + slot] = (dot_tn(x[tab[UR, n]], delta[cols + tab[UC, n]]) * live(1, n)).astype(BF)
            return 0

        lax.fori_loop(0, 4, body, 0)
        core_send(k, 0)

    run(OUT, SLOTS, 0, lambda v: dot_nn(hid[v & 63], w[v >> 6]))
    put(0, 0, OUT)
    x_start(0)
    lax.fori_loop(0, 8, down_grads, 0)
    for k in (2, 1, 3, 0):
        core_send(k, 1)
    mine(groups[3] + groups[4] + groups[5] + groups[6], 1)
    theirs(sum(groups, ()), 1, wait=False)
    run(HID, SLOTS, 2 * SLOTS, lambda n: p[2 * SLOTS + n])

    def act_grad(c, _):
        hg = pick(2 * SLOTS, HID, c)
        delta[c] = (hg * p[c]).astype(BF)
        delta[cols + c] = (hg * p[cols + c]).astype(BF)
        return 0

    lax.fori_loop(0, cols, act_grad, 0)
    for k in (2, 1, 3, 0):
        y_start(k, 1)
    in_grads(2)
    in_grads(1)
    x_pass(0)
    x_pass(1)
    for k in (2, 1, 3, 0):
        y_pass(k, 1)
    run(INP, 2 * SLOTS, SLOTS, lambda v: dot_nt(delta[v & 63], w[v >> 6]))
    put(1, SLOTS, INP)
    x_start(1)
    y_start(2, 0)
    in_grads(3)
    y_start(1, 0)
    in_grads(0)
    y_start(3, 0)
    for k in (2, 1, 3, 0):
        y_end(k, 1)
    y_start(0, 0)
    x_end(0)
    y_pass(2, 0)
    x_end(1)
    z_pass(1)
    y_pass(1, 0)
    x_pass(2)
    y_pass(3, 0)
    y_end(2, 0)
    x_pass(3)
    y_pass(0, 0)
    y_end(1, 0)
    y_end(3, 0)
    l_end(0)
    l_end(1)
    z_end(1)
    z_pass(0)
    y_end(0, 0)
    x_end(2)
    x_end(3)
    z_end(0)
    l_end(2)
    l_end(3)
    for copy in results:
        copy.wait()
    send.finish()


def finish_kernel(*refs):
    for src, dst in zip(refs[:5], refs[5:]):
        dst[...] = src[...]


def shards(tokens, cotangent, gate_blocks, up_blocks, down_blocks, gate_where, up_where, down_where, block_counts):
    cols = FF // (BK * lax.axis_size("tensor"))
    toks = tokens.shape[0]
    dma = pltpu.SemaphoreType.DMA
    shapes = (
        jax.ShapeDtypeStruct((toks, 1024), BF),
        jax.ShapeDtypeStruct((toks, 1024), BF),
        jax.ShapeDtypeStruct((1, 2, BK, BK), BF),
        jax.ShapeDtypeStruct((1, 2, BK, BK), BF),
        jax.ShapeDtypeStruct((1, 2, BK, BK), BF),
    )
    counts = block_counts.reshape(3)
    table = pl.pallas_call(
        table_kernel,
        out_shape=jax.ShapeDtypeStruct((26, BK), jnp.int32),
        in_specs=[SM, VM, VM, VM],
        out_specs=VM,
    )(counts, gate_where, up_where, down_where)
    results = pl.pallas_call(
        layer_kernel,
        out_shape=shapes,
        in_specs=[SM, SM] + [ANY] * 5,
        out_specs=(ANY,) * 5,
        scratch_shapes=[
            pltpu.VMEM((tokens.shape[1] // BK, toks, BK), BF),
            pltpu.VMEM((tokens.shape[1] // BK, toks, BK), BF),
            pltpu.VMEM((192, BK, BK), BF),
            pltpu.VMEM((3 * SLOTS, BK, BK), F32),
            pltpu.VMEM((3 * SLOTS, BK, BK), F32),
            pltpu.VMEM((cols, BK, BK), BF),
            pltpu.VMEM((2 * cols, BK, BK), BF),
            pltpu.VMEM((4, 8, toks, 512), BF),
            pltpu.VMEM((32, 6, BK, BK), BF),
            pltpu.VMEM((4, 4, 6, BK, BK), BF),
            pltpu.VMEM((4, 6, BK, BK), BF),
            pltpu.VMEM((4, 2, 6, BK, BK), BF),
            pltpu.VMEM((4, 6, BK, BK), BF),
            pltpu.VMEM((6, BK, BK), BF),
            pltpu.VMEM((2, 6, BK, BK), BF),
            pltpu.VMEM((4, 2, toks, 512), BF),
            pltpu.VMEM((4, 2, 2, toks, 512), BF),
            pltpu.VMEM((4, toks, 512), BF),
            pltpu.VMEM((4, toks, 512), BF),
            pltpu.VMEM((4, toks, 512), BF),
            pltpu.VMEM((6, BK, BK), BF),
            dma((5,)),
            dma((7,)),
            dma((256,)),
            dma((2, 4, 2)),
            dma((2, 4, 4, 2)),
            dma((2, 4, 4, 2)),
            dma((2, 4, 4)),
            dma((2, 4, 2)),
            dma((2, 4, 2, 2)),
            dma((2, 2)),
            dma((2, 2, 2)),
            dma((4, 2)),
            dma((4, 2, 2)),
            dma((4,)),
        ],
        compiler_params=pltpu.CompilerParams(
            collective_id=0, has_side_effects=True, vmem_limit_bytes=67043328
        ),
    )(
        counts, table, tokens, cotangent, gate_blocks, up_blocks, down_blocks,
    )
    return pl.pallas_call(
        finish_kernel, out_shape=shapes, in_specs=[VM] * 5, out_specs=(VM,) * 5,
    )(*results)


def solution(mesh):
    placed = (
        P("fsdp", None),
        P("fsdp", None),
        P("tensor", "fsdp", None, None),
        P("tensor", "fsdp", None, None),
        P("tensor", "fsdp", None, None),
        P("tensor", None),
        P("tensor", None),
        P("tensor", None),
        P(None, "tensor"),
    )
    return jax.shard_map(
        shards,
        mesh=mesh,
        in_specs=placed,
        out_specs=(
            P("fsdp", "tensor"),
            P("fsdp", "tensor"),
            P("tensor", "fsdp", None, None),
            P("tensor", "fsdp", None, None),
            P("tensor", "fsdp", None, None),
        ),
        check_vma=False,
    )
```

```python
import jax
import jax.numpy as jnp
from jax import lax
from jax.experimental import pallas as pl
from jax.experimental.pallas import tpu as pltpu
from jax.sharding import PartitionSpec as P

FF = 14336
BK = 128
BF = jnp.bfloat16
F32 = jnp.float32
MESH = pl.DeviceIdType.MESH
VM = pl.BlockSpec(memory_space=pltpu.VMEM)
SM = pl.BlockSpec(memory_space=pltpu.SMEM)
ANY = pl.BlockSpec(memory_space=pl.ANY)
NZ, NY = 4, 4
HALF = (slice(0, 3), slice(3, 6))


class Place:
    def __init__(self):
        rem, div = lax.rem, lax.div
        self.f = lax.axis_index("fsdp")
        self.t = lax.axis_index("tensor")
        self.c = rem(self.f, 2)
        chip = div(self.f, 2)
        y, zh = rem(chip, 4), div(chip, 4)
        self.zl = div(self.t, 4)
        x = rem(self.t, 4)
        self.ys = [rem(y + j, 4) for j in range(4)]
        self.zs = [rem(zh + k, 4) for k in range(4)]
        self.xs = [rem(x + m, 4) for m in range(4)]
        self.same = [[(self.zs[k] * 4 + self.ys[j]) * 2 + self.c for j in range(4)] for k in range(4)]
        self.twin = [[(self.zs[k] * 4 + self.ys[j]) * 2 + (1 - self.c) for j in range(4)] for k in range(4)]
        self.line = [self.zl * 4 + v for v in self.xs]
        self.across = (1 - self.zl) * 4 + x

    def fs(self, k=0, j=0):
        return self.same[k % 4][j % 4]

    def dev(self, k=0, j=0, flip=False):
        return ((self.twin if flip else self.same)[k % 4][j % 4], self.t)

    def tdev(self, m=0, flip=False):
        return (self.f, self.across if flip else self.line[m % 4])


class Sender:
    def __init__(self, sems):
        self.sems = sems
        self.sent = []

    def __call__(self, src, dst, recv, dev):
        copy = pltpu.make_async_remote_copy(
            src_ref=src,
            dst_ref=dst,
            send_sem=self.sems.at[len(self.sent)],
            recv_sem=recv,
            device_id=dev,
            device_id_type=MESH,
        )
        copy.start()
        self.sent.append(copy)

    def finish(self):
        for copy in self.sent:
            copy.wait_send()


def arrive(ref, sem):
    pltpu.make_async_copy(ref, ref, sem).wait()


def greet(devs):
    barrier = pltpu.get_barrier_semaphore()
    for dev in devs:
        pl.semaphore_signal(barrier, inc=1, device_id=dev, device_id_type=MESH)
    return lambda: pl.semaphore_wait(barrier, len(devs))


ORDER, KEEP, END, SOME = 0, 5, 10, 15
GR, GC, UR, UC, DF, DD = range(20, 26)
GATE, UP, HID, OUT, INP = range(5)
UNROLL = 8
SLOTS = 64
FLOWS = ((0, 2), (4, 1))


def half(fl, h, base=0):
    first, size = FLOWS[fl]
    return pl.ds(base + first + size * h, size)


def whole(fl):
    first, size = FLOWS[fl]
    return pl.ds(first, 2 * size)


def dot_nn(a, b):
    return lax.dot_general(a, b, (((1,), (0,)), ((), ())), preferred_element_type=F32)


def dot_nt(a, b):
    return lax.dot_general(a, b, (((1,), (1,)), ((), ())), preferred_element_type=F32)


def dot_tn(a, b):
    return lax.dot_general(a, b, (((0,), (0,)), ((), ())), preferred_element_type=F32)


def split14(v):
    q = (v * 4682) >> 16
    return q, v - q * 14


def make_table(counts, gw, uw, dw, tab):
    n64 = lax.broadcasted_iota(jnp.int32, (1, SLOTS), 1)
    gr, gc = split14(gw[...])
    ur, uc = split14(uw[...])
    df, dd = dw[...] >> 6, dw[...] & 63
    base = (n64 >> 1) * 6 + (n64 & 1)

    def key(k, v):
        return jnp.where(n64 < counts[k], v, 64)

    def wide(v, fill):
        return jnp.concatenate([v, jnp.full((1, SLOTS), fill, jnp.int32)], axis=1)

    keys = (
        wide(key(0, gc), 65),
        wide(key(1, uc), 65),
        wide(key(2, df), 65),
        wide(key(2, dd), 65),
        jnp.concatenate([key(0, gr), key(1, ur)], axis=1),
    )
    loads = (
        wide(n64, 0),
        wide(n64, 0),
        wide(n64, 0),
        wide((base + 4) * 64 + df, 0),
        jnp.concatenate([base * 64 + gc, (base + 2) * 64 + uc + 14], axis=1),
    )
    row_i = lax.broadcasted_iota(jnp.int32, (BK, BK), 0)
    col_i = lax.broadcasted_iota(jnp.int32, (BK, BK), 1)
    lane = lax.broadcasted_iota(jnp.int32, (1, BK), 1)
    for k in range(5):
        by_lane = jnp.broadcast_to(keys[k], (BK, BK))
        by_row = by_lane.T
        code = jnp.broadcast_to(loads[k] * 128 + keys[k], (BK, BK)).T
        before = (by_row < by_lane) | ((by_row == by_lane) & (row_i < col_i))
        rank = jnp.sum(before.astype(jnp.int32), axis=0, keepdims=True)
        rank_row = jnp.broadcast_to(rank, (BK, BK)).T
        both = jnp.sum(jnp.where(rank_row == col_i, code, 0), axis=0, keepdims=True)
        skey = both & 127
        tab[ORDER + k : ORDER + k + 1, :] = both >> 7
        same = (skey == pltpu.roll(skey, 1, 1)) & (lane > 0)
        tab[KEEP + k : KEEP + k + 1, :] = same.astype(jnp.int32)
        upto = jnp.sum((by_row <= col_i).astype(jnp.int32), axis=0, keepdims=True)
        some = jnp.sum((by_row == col_i).astype(jnp.int32), axis=0, keepdims=True)
        tab[END + k : END + k + 1, :] = jnp.maximum(upto - 1, 0)
        tab[SOME + k : SOME + k + 1, :] = (some > 0).astype(jnp.int32)
    for i, v in enumerate((gr, gc, ur, uc, df, dd)):
        tab[GR + i : GR + i + 1, :] = wide(v, 0)


def add2(a, b):
    return (a.astype(F32) + b.astype(F32)).astype(BF)


def add3(a, b, c):
    return a.astype(F32) + b.astype(F32) + c.astype(F32)


def layer_kernel(
    cnt, gwv, uwv, dwv, x_hbm, g_hbm, gate_hbm, up_hbm, down_hbm,
    out_hbm, ing_hbm, gg_hbm, ug_hbm, dg_hbm,
    x, g, w, p, s, hid, delta, tabv, tab,
    o, d, pbuf, y2, yr, bbuf, z2, zr, x2, xr, tz, zlb, fin, fing,
    lsem, tsem, fsem, ssem, rz, ry, rp, rq, ry2, ryr, rz2, rzr, rx2, rxr, rl,
):
    me = Place()
    own = me.fs()
    cols = hid.shape[0]
    met = greet([me.dev(1), me.dev(3), me.dev(0, 1), me.dev(0, 3), me.dev(flip=True),
                 me.tdev(1), me.tdev(3), me.tdev(flip=True)])
    local = [
        pltpu.make_async_copy(src.at[0], w.at[pl.ds(own * 6 + 2 * i, 2)], lsem.at[i])
        for i, src in enumerate((gate_hbm, up_hbm, down_hbm))
    ]
    for copy in local:
        copy.start()

    def bring(b, _):
        at = pl.ds(pl.multiple_of(b * BK, BK), BK)
        pltpu.make_async_copy(x_hbm.at[:, at], x.at[b], lsem.at[3]).start()
        pltpu.make_async_copy(g_hbm.at[:, at], g.at[b], lsem.at[4]).start()
        return 0

    lax.fori_loop(0, x.shape[0], bring, 0)
    met()
    for copy in local:
        copy.wait()
    send = Sender(ssem)

    def piece(k, j, fl, h):
        return w.at[half(fl, h, me.fs(k, j) * 6)]

    def to_z(k, fl, h, step):
        send(piece(k, 0, fl, h), piece(k, 0, fl, h), rz.at[fl, (k - step) % 4, h], me.dev(step))

    def to_y(k, j, fl, h, step):
        send(piece(k, j, fl, h), piece(k, j, fl, h), ry.at[fl, k, (j - step) % 4, h], me.dev(0, step))

    def to_core(k, j, fl, h):
        send(piece(k, j, fl, h), piece(k, j, fl, h), rp.at[fl, k, j, h], me.dev(flip=True))

    def on_y(k, j, fl, h):
        arrive(piece(k, j, fl, h), ry.at[fl, k, j, h])
        if j == 3 and h == 0:
            to_y(k, j, fl, h, 1)
        if j == 1 and h == 1:
            to_y(k, j, fl, h, -1)
        to_core(k, j, fl, h)

    def on_z(k, fl, h):
        arrive(piece(k, 0, fl, h), rz.at[fl, k, h])
        if k == 3 and h == 0:
            to_z(k, fl, h, 1)
        if k == 1 and h == 1:
            to_z(k, fl, h, -1)
        to_y(k, 0, fl, h, 1)
        to_y(k, 0, fl, h, -1)
        to_core(k, 0, fl, h)

    def begin(fl):
        for h in (0, 1):
            to_z(0, fl, h, 1)
            to_z(0, fl, h, -1)
            to_y(0, 0, fl, h, 1)
            to_y(0, 0, fl, h, -1)
            to_core(0, 0, fl, h)

    def products(f, fl):
        for slot in (0, 1):
            n = 2 * f + slot
            if fl == 0:
                p[n] = dot_nn(x[tab[GR, n]], w[f * 6 + slot])
                p[SLOTS + n] = dot_nn(x[tab[UR, n]], w[f * 6 + 2 + slot])
            else:
                p[2 * SLOTS + n] = dot_nt(g[tab[DD, n]], w[f * 6 + 4 + slot])

    def mine(chunks, fl):
        for k, j in chunks:
            products(me.fs(k, j), fl)

    def wait_theirs(chunks, fl):
        for k, j in chunks:
            for h in (0, 1):
                arrive(w.at[half(fl, h, me.twin[k][j] * 6)], rp.at[fl, k, j, h])

    def theirs(chunks, fl, wait=True):
        if wait:
            wait_theirs(chunks, fl)
        for k, j in chunks:
            products(me.twin[k][j], fl)

    groups = (
        ((0, 0),),
        ((0, 3), (0, 1), (3, 0), (1, 0)),
        ((2, 0), (0, 2)),
        ((3, 3), (3, 1), (1, 3), (1, 1)),
        ((3, 2), (1, 2)),
        ((2, 3), (2, 1)),
        ((2, 2),),
    )

    def take(i, fl):
        for h in (0, 1):
            for k, j in groups[i]:
                if j == 0:
                    on_z(k, fl, h)
                else:
                    on_y(k, j, fl, h)

    def run(kind, count, first, term, wide=UNROLL):
        def body(step, acc):
            for u in range(wide):
                i = step * wide + u
                keep = tab[KEEP + kind, i].astype(F32)
                acc = acc * keep + term(tab[ORDER + kind, i])
                s[first + i] = acc
            return acc

        lax.fori_loop(0, count // wide, body, jnp.zeros((BK, BK), F32))

    def pick(first, kind, c):
        return s[first + tab[END + kind, c]] * tab[SOME + kind, c].astype(F32)

    begin(0)
    begin(1)
    make_table(cnt, gwv, uwv, dwv, tabv)
    table = pltpu.make_async_copy(tabv, tab, tsem)
    table.start()
    take(1, 0)
    table.wait()
    arrive(x, lsem.at[3])
    mine(groups[0] + groups[1], 0)
    take(2, 0)
    take(1, 1)
    theirs(groups[0], 0)
    mine(groups[2], 0)
    take(3, 0)
    take(2, 1)
    theirs(groups[1], 0)
    mine(groups[3], 0)
    take(4, 0)
    theirs(groups[2], 0)
    mine(groups[4], 0)
    take(5, 0)
    take(3, 1)
    theirs(groups[3], 0)
    mine(groups[5], 0)
    take(6, 0)
    theirs(groups[4], 0)
    mine(groups[6], 0)
    take(4, 1)
    theirs(groups[5] + groups[6], 0)
    run(GATE, SLOTS, 0, lambda n: p[n])
    run(UP, SLOTS, SLOTS, lambda n: p[SLOTS + n])

    def act(c, _):
        gate = pick(0, GATE, c)
        up = pick(SLOTS, UP, c)
        sig = jax.nn.sigmoid(gate)
        silu = gate * sig
        hid[c] = (silu * up).astype(BF)
        p[c] = up * sig * (1.0 + gate * (1.0 - sig))
        p[cols + c] = silu
        return 0

    lax.fori_loop(0, cols, act, 0)
    take(5, 1)
    arrive(g, lsem.at[4])
    mine(groups[0] + groups[1] + groups[2], 1)
    take(6, 1)
    wait_theirs(sum(groups, ()), 1)

    results = []

    def result(src, dst):
        copy = pltpu.make_async_copy(src, dst, fsem.at[len(results)])
        copy.start()
        results.append(copy)

    def opiece(b, zl, m):
        return o.at[b, zl * 4 + me.xs[m % 4]]

    def put(a, first, kind):
        def body(q, _):
            for r in range(8):
                at = slice(r % 4 * BK, (r % 4 + 1) * BK)
                o[2 * a + r // 4, q, :, at] = pick(first, kind, q * 8 + r).astype(BF)
            return 0

        lax.fori_loop(0, 8, body, 0)

    def x_start(bs):
        for b in bs:
            send(opiece(b, 0, 2), x2.at[b, 0], rx2.at[b, 0], me.tdev(1))
            send(opiece(b, 1, 2), x2.at[b, 1], rx2.at[b, 1], me.tdev(-1))
        for b in bs:
            send(opiece(b, 1, 1), xr.at[b, 0, 1], rxr.at[b, 0, 1], me.tdev(1))
            send(opiece(b, 0, -1), xr.at[b, 1, 0], rxr.at[b, 1, 0], me.tdev(-1))

    def x_pass(b):
        for h, m in ((0, 1), (1, -1)):
            arrive(x2.at[b, h], rx2.at[b, h])
            x2[b, h] = add2(o[b, h * 4 + me.xs[m % 4]], x2[b, h])
            send(x2.at[b, h], xr.at[b, h, h], rxr.at[b, h, h], me.tdev(m))

    def x_end(b):
        for e in (0, 1):
            for h in (0, 1):
                arrive(xr.at[b, e, h], rxr.at[b, e, h])
        other = 1 - me.zl
        tz[b] = add3(o[b, me.across], xr[b, 0, other], xr[b, 1, other]).astype(BF)
        send(tz.at[b], zlb.at[b], rl.at[b], me.tdev(flip=True))

    def l_end(b):
        own_sum = add3(o[b, me.line[0]], xr[b, 0, me.zl], xr[b, 1, me.zl])
        arrive(zlb.at[b], rl.at[b])
        fin[b] = (own_sum + zlb[b].astype(F32)).astype(BF)
        result(fin.at[b], (out_hbm, ing_hbm)[b // 2].at[:, pl.ds(b % 2 * 512, 512)])

    def core_send(k, fl):
        for j in (2, 1, 3, 0):
            send(d.at[me.twin[k][j], whole(fl)], pbuf.at[k, j, whole(fl)], rq.at[fl, k, j], me.dev(flip=True))

    def core_sum(k, j, fl):
        arrive(pbuf.at[k, j, whole(fl)], rq.at[fl, k, j])
        f = me.fs(k, j)
        d[f, whole(fl)] = add2(d[f, whole(fl)], pbuf[k, j, whole(fl)])

    def y_start(k, fl):
        core_sum(k, 2, fl)
        far = me.fs(k, 2)
        send(d.at[far, half(fl, 0)], y2.at[k, half(fl, 0)], ry2.at[fl, k, 0], me.dev(0, 1))
        send(d.at[far, half(fl, 1)], y2.at[k, half(fl, 1)], ry2.at[fl, k, 1], me.dev(0, -1))
        core_sum(k, 1, fl)
        send(d.at[me.fs(k, 1), half(fl, 1)], yr.at[k, 0, half(fl, 1)], ryr.at[fl, k, 0, 1], me.dev(0, 1))
        core_sum(k, 3, fl)
        send(d.at[me.fs(k, 3), half(fl, 0)], yr.at[k, 1, half(fl, 0)], ryr.at[fl, k, 1, 0], me.dev(0, -1))
        core_sum(k, 0, fl)

    def y_pass(k, fl):
        for h, j in ((0, 1), (1, 3)):
            at = half(fl, h)
            arrive(y2.at[k, at], ry2.at[fl, k, h])
            y2[k, at] = add2(d[me.fs(k, j), at], y2[k, at])
            send(y2.at[k, at], yr.at[k, h, at], ryr.at[fl, k, h, h], me.dev(0, j))

    def y_end(k, fl):
        for e in (0, 1):
            for h in (0, 1):
                arrive(yr.at[k, e, half(fl, h)], ryr.at[fl, k, e, h])
        at = whole(fl)
        bbuf[k, at] = add3(d[me.fs(k, 0), at], yr[k, 0, at], yr[k, 1, at]).astype(BF)
        if k == 2:
            send(bbuf.at[2, half(fl, 0)], z2.at[half(fl, 0)], rz2.at[fl, 0], me.dev(1))
            send(bbuf.at[2, half(fl, 1)], z2.at[half(fl, 1)], rz2.at[fl, 1], me.dev(-1))
        if k == 1:
            send(bbuf.at[1, half(fl, 1)], zr.at[0, half(fl, 1)], rzr.at[fl, 0, 1], me.dev(1))
        if k == 3:
            send(bbuf.at[3, half(fl, 0)], zr.at[1, half(fl, 0)], rzr.at[fl, 1, 0], me.dev(-1))

    def z_pass(fl):
        for h, k in ((0, 1), (1, 3)):
            at = half(fl, h)
            arrive(z2.at[at], rz2.at[fl, h])
            z2[at] = add2(bbuf[k, at], z2[at])
            send(z2.at[at], zr.at[h, at], rzr.at[fl, h, h], me.dev(k))

    def z_end(fl):
        for e in (0, 1):
            for h in (0, 1):
                arrive(zr.at[e, half(fl, h)], rzr.at[fl, e, h])
        at = whole(fl)
        fing[at] = add3(bbuf[0, at], zr[0, at], zr[1, at]).astype(BF)
        for b in (0, 1) if fl == 0 else (2,):
            result(fing.at[pl.ds(2 * b, 2)], (gg_hbm, ug_hbm, dg_hbm)[b].at[0])

    def live(k, n):
        return (n < cnt[k]).astype(F32)

    def down_grads(i, _):
        for e in range(4):
            f = i * 4 + e
            for slot in (0, 1):
                n = 2 * f + slot
                d[f, 4 + slot] = (dot_tn(hid[tab[DF, n]], g[tab[DD, n]]) * live(2, n)).astype(BF)
        return 0

    def in_grads(k):
        def body(i, _):
            for e in (0, 1):
                f = me.zs[k] * 8 + i * 2 + e
                for slot in (0, 1):
                    n = 2 * f + slot
                    d[f, slot] = (dot_tn(x[tab[GR, n]], delta[tab[GC, n]]) * live(0, n)).astype(BF)
                    d[f, 2 + slot] = (dot_tn(x[tab[UR, n]], delta[cols + tab[UC, n]]) * live(1, n)).astype(BF)
            return 0

        lax.fori_loop(0, 4, body, 0)
        core_send(k, 0)

    def act_grad(c, _):
        hg = pick(2 * SLOTS, HID, c)
        delta[c] = (hg * p[c]).astype(BF)
        delta[cols + c] = (hg * p[cols + c]).astype(BF)
        return 0

    run(OUT, SLOTS, 0, lambda v: dot_nn(hid[v & 63], w[v >> 6]), 16)
    put(0, 0, OUT)
    x_start((0, 1))
    lax.fori_loop(0, 8, down_grads, 0)
    for k in (2, 1, 3, 0):
        core_send(k, 1)
    mine(groups[3] + groups[4] + groups[5] + groups[6], 1)
    theirs(sum(groups, ()), 1, wait=False)
    y_start(2, 1)
    y_start(1, 1)
    run(HID, SLOTS, 2 * SLOTS, lambda n: p[2 * SLOTS + n])
    lax.fori_loop(0, cols, act_grad, 0)
    y_start(3, 1)
    y_start(0, 1)
    in_grads(2)
    in_grads(1)
    x_pass(0)
    x_pass(1)
    for k in (2, 1, 3, 0):
        y_pass(k, 1)
    y_start(2, 0)
    run(INP, 2 * SLOTS, SLOTS, lambda v: dot_nt(delta[v & 63], w[v >> 6]), 16)
    put(1, SLOTS, INP)
    x_start((2, 3))
    y_start(1, 0)
    in_grads(3)
    in_grads(0)
    y_start(3, 0)
    for k in (2, 1, 3, 0):
        y_end(k, 1)
    y_start(0, 0)
    y_pass(2, 0)
    x_end(0)
    x_end(1)
    y_pass(1, 0)
    z_pass(1)
    x_pass(2)
    x_pass(3)
    y_pass(3, 0)
    y_end(2, 0)
    l_end(0)
    l_end(1)
    y_pass(0, 0)
    y_end(1, 0)
    y_end(3, 0)
    x_end(2)
    z_pass(0)
    z_end(1)
    y_end(0, 0)
    x_end(3)
    l_end(2)
    z_end(0)
    l_end(3)
    for copy in results:
        copy.wait()
    send.finish()


def finish_kernel(*refs):
    for src, dst in zip(refs[:5], refs[5:]):
        dst[...] = src[...]


def shards(tokens, cotangent, gate_blocks, up_blocks, down_blocks, gate_where, up_where, down_where, block_counts):
    cols = FF // (BK * lax.axis_size("tensor"))
    toks = tokens.shape[0]
    dma = pltpu.SemaphoreType.DMA
    shapes = (
        jax.ShapeDtypeStruct((toks, 1024), BF),
        jax.ShapeDtypeStruct((toks, 1024), BF),
        jax.ShapeDtypeStruct((1, 2, BK, BK), BF),
        jax.ShapeDtypeStruct((1, 2, BK, BK), BF),
        jax.ShapeDtypeStruct((1, 2, BK, BK), BF),
    )
    counts = block_counts.reshape(3)
    results = pl.pallas_call(
        layer_kernel,
        out_shape=shapes,
        in_specs=[SM, VM, VM, VM] + [ANY] * 5,
        out_specs=(ANY,) * 5,
        scratch_shapes=[
            pltpu.VMEM((tokens.shape[1] // BK, toks, BK), BF),
            pltpu.VMEM((tokens.shape[1] // BK, toks, BK), BF),
            pltpu.VMEM((192, BK, BK), BF),
            pltpu.VMEM((3 * SLOTS, BK, BK), F32),
            pltpu.VMEM((3 * SLOTS, BK, BK), F32),
            pltpu.VMEM((cols, BK, BK), BF),
            pltpu.VMEM((2 * cols, BK, BK), BF),
            pltpu.VMEM((26, BK), jnp.int32),
            pltpu.SMEM((26, BK), jnp.int32),
            pltpu.VMEM((4, 8, toks, 512), BF),
            pltpu.VMEM((32, 6, BK, BK), BF),
            pltpu.VMEM((4, 4, 6, BK, BK), BF),
            pltpu.VMEM((4, 6, BK, BK), BF),
            pltpu.VMEM((4, 2, 6, BK, BK), BF),
            pltpu.VMEM((4, 6, BK, BK), BF),
            pltpu.VMEM((6, BK, BK), BF),
            pltpu.VMEM((2, 6, BK, BK), BF),
            pltpu.VMEM((4, 2, toks, 512), BF),
            pltpu.VMEM((4, 2, 2, toks, 512), BF),
            pltpu.VMEM((4, toks, 512), BF),
            pltpu.VMEM((4, toks, 512), BF),
            pltpu.VMEM((4, toks, 512), BF),
            pltpu.VMEM((6, BK, BK), BF),
            dma((5,)),
            dma,
            dma((7,)),
            dma((256,)),
            dma((2, 4, 2)),
            dma((2, 4, 4, 2)),
            dma((2, 4, 4, 2)),
            dma((2, 4, 4)),
            dma((2, 4, 2)),
            dma((2, 4, 2, 2)),
            dma((2, 2)),
            dma((2, 2, 2)),
            dma((4, 2)),
            dma((4, 2, 2)),
            dma((4,)),
        ],
        compiler_params=pltpu.CompilerParams(
            collective_id=0, has_side_effects=True, vmem_limit_bytes=67043328
        ),
    )(
        counts, gate_where, up_where, down_where, tokens, cotangent, gate_blocks, up_blocks, down_blocks,
    )
    return pl.pallas_call(
        finish_kernel, out_shape=shapes, in_specs=[VM] * 5, out_specs=(VM,) * 5,
    )(*results)


def solution(mesh):
    placed = (
        P("fsdp", None),
        P("fsdp", None),
        P("tensor", "fsdp", None, None),
        P("tensor", "fsdp", None, None),
        P("tensor", "fsdp", None, None),
        P("tensor", None),
        P("tensor", None),
        P("tensor", None),
        P(None, "tensor"),
    )
    return jax.shard_map(
        shards,
        mesh=mesh,
        in_specs=placed,
        out_specs=(
            P("fsdp", "tensor"),
            P("fsdp", "tensor"),
            P("tensor", "fsdp", None, None),
            P("tensor", "fsdp", None, None),
            P("tensor", "fsdp", None, None),
        ),
        check_vma=False,
    )
```
